16 devices in a mesh: tp: 2 (over z), dp: 8 (over y, x, core).
Axes of the slice: x: 2, y: 2, z: 2, core: 2. Of those that a mesh axis runs over, the one named last changes fastest.
Arguments:
- hidden_in: bfloat16 [4096, 4096], P('dp')
- labels: int32 [4096], P('dp')
- loss_mask: int32 [4096], P('dp')
- norm_gamma: bfloat16 [4096], replicated
- w_out: bfloat16 [4096, 32000], P(None, 'tp')
Outputs:
- output 1: float32 [], replicated
- output 2: bfloat16 [4096, 4096], P('dp')
- output 3: float32 [4096, 32000], P('dp', 'tp')
- output 4: float32 [4096], replicated
All inputs are finite; a program needn't handle non-finite values.
Results may differ from the reference program's by a relative error of at most 0.001.
Values sent between devices are 32-bit elements.
A program may use at most 1 GiB of HBM per device.

```python
import jax
import jax.numpy as jnp
from jax import lax

HIDDEN_SIZE = 4096
VOCAB_SIZE = 32000
NUM_TOKENS = 4096
NORM_EPS = 1e-5


def setup_inputs(seed: int = 0) -> dict:
    key = jax.random.key(seed)
    k_x, k_gamma, k_w, k_lab, k_mask = jax.random.split(key, 5)
    hidden_in = jax.random.normal(k_x, (NUM_TOKENS, HIDDEN_SIZE), jnp.float32).astype(jnp.bfloat16)
    norm_gamma = (1.0 + 0.5 * jax.random.normal(k_gamma, (HIDDEN_SIZE,), jnp.float32)).astype(jnp.bfloat16)
    w_out = (3.0 * HIDDEN_SIZE ** -0.5 * jax.random.normal(k_w, (HIDDEN_SIZE, VOCAB_SIZE), jnp.float32)).astype(jnp.bfloat16)
    labels = jax.random.randint(k_lab, (NUM_TOKENS,), 0, VOCAB_SIZE, jnp.int32)
    labels = labels.at[0].set(0).at[NUM_TOKENS - 1].set(VOCAB_SIZE - 1)
    thresh = 20 + (60 * jnp.arange(NUM_TOKENS, dtype=jnp.int32)) // NUM_TOKENS
    draws = jax.random.randint(k_mask, (NUM_TOKENS,), 0, 100, jnp.int32)
    loss_mask = (draws < thresh).astype(jnp.int32).at[0].set(1)
    return {"hidden_in": hidden_in, "labels": labels, "loss_mask": loss_mask, "norm_gamma": norm_gamma, "w_out": w_out}


def reference(hidden_in, labels, loss_mask, norm_gamma, w_out):
    hid_f32 = hidden_in.astype(jnp.float32)
    gain_f32 = norm_gamma.astype(jnp.float32)
    inv_rms = lax.rsqrt(jnp.mean(hid_f32 * hid_f32, axis=-1, keepdims=True) + NORM_EPS)
    x_hat = hid_f32 * inv_rms
    normed = (x_hat * gain_f32).astype(jnp.bfloat16)
    logits = jnp.dot(normed, w_out, preferred_element_type=jnp.float32)
    row_max = jnp.max(logits, axis=-1, keepdims=True)
    log_z = row_max + jnp.log(jnp.sum(jnp.exp(logits - row_max), axis=-1, keepdims=True))
    one_hot = labels[:, None] == jnp.arange(VOCAB_SIZE, dtype=jnp.int32)[None, :]
    target = jnp.sum(jnp.where(one_hot, logits, 0.0), axis=-1, keepdims=True)
    mask_f32 = loss_mask.astype(jnp.float32)[:, None]
    count = jnp.sum(mask_f32)
    loss = jnp.sum(mask_f32 * (log_z - target)) / count
    tok_scale = mask_f32 / count
    d_logits = ((jnp.exp(logits - log_z) - one_hot.astype(jnp.float32)) * tok_scale).astype(jnp.bfloat16)
    d_w_out = jnp.dot(normed.T, d_logits, preferred_element_type=jnp.float32)
    d_normed = jnp.dot(d_logits, w_out.T, preferred_element_type=jnp.float32)
    d_gamma = jnp.sum(d_normed * x_hat, axis=0)
    d_hat = d_normed * gain_f32
    d_hidden = (inv_rms * (d_hat - x_hat * jnp.mean(d_hat * x_hat, axis=-1, keepdims=True))).astype(jnp.bfloat16)
    return (loss, d_hidden, d_w_out, d_gamma)
```

```python
import functools

import jax
import jax.numpy as jnp
from jax import lax
from jax.experimental import pallas as pl
from jax.experimental.pallas import tpu as pltpu
from jax.sharding import PartitionSpec as P

NORM_EPS = 1e-5
F32, BF16, I32 = jnp.float32, jnp.bfloat16, jnp.int32
VMEM_LIMIT = 64 * 1024 * 1024 - 64 * 1024
LANES = 128
ROWS = 8
NT = (((1,), (1,)), ((), ()))


def call(body, **kw):
    cost = kw.pop("cost")
    return pl.pallas_call(body, compiler_params=pltpu.CompilerParams(vmem_limit_bytes=VMEM_LIMIT), cost_estimate=pl.CostEstimate(flops=cost[0], bytes_accessed=cost[1], transcendentals=0), **kw)


def whole(shape):
    return pl.BlockSpec(shape, lambda *_: (0,) * len(shape))


def columns(rows):
    return jnp.transpose(jnp.concatenate([rows] * (LANES // ROWS), axis=0))


def softmax_grad(z, cols, first):
    hot = lax.broadcasted_iota(I32, z.shape, 1) + first == cols[:, 2:3].astype(I32)
    return ((jnp.exp(z - cols[:, 0:1]) - hot.astype(F32)) * cols[:, 1:2]).astype(BF16)


def token_columns(picked, aux_own, aux_x, aux_y, aux_d):
    count = aux_own[3:4, 0:1] + aux_x[3:4, 0:1] + aux_y[3:4, 0:1] + aux_d[3:4, 0:1]
    row = lax.broadcasted_iota(I32, picked.shape, 0)
    return columns(jnp.where(row == 1, picked / count, picked))


def prep_body(x_ref, gain_ref, hat_ref, n_ref, inv_ref):
    x = x_ref[...].astype(F32)
    inv = lax.rsqrt(jnp.mean(x * x, axis=-1, keepdims=True) + NORM_EPS)
    hat = x * inv
    hat_ref[...] = hat
    n_ref[...] = (hat * gain_ref[...]).astype(BF16)
    inv_ref[...] = inv


def prep_half(x, gain, part, block=128):
    t, h = x.shape
    half = t // 2
    steps = half // block
    return call(
        prep_body,
        grid=(steps,),
        in_specs=[pl.BlockSpec((block, h), lambda j: (j + part * steps, 0)), whole((1, h))],
        out_specs=[pl.BlockSpec((block, h), lambda j: (j, 0)), pl.BlockSpec((block, h), lambda j: (j, 0)), pl.BlockSpec((block, 1), lambda j: (j, 0))],
        out_shape=[jax.ShapeDtypeStruct((half, h), F32), jax.ShapeDtypeStruct((half, h), BF16), jax.ShapeDtypeStruct((half, 1), F32)],
        cost=(8 * half * h, 8 * half * h),
    )(x, gain)


def own_body(n0_ref, n1_ref, w_ref, lab_ref, z_ref, st_ref, n_sc, lab_sc, m_sc, s_sc, t_sc, *, tile, chunk, vocab):
    j = pl.program_id(0)
    half = n0_ref.shape[0]

    @pl.when(j == 0)
    def _():
        n_sc[:half, :] = n0_ref[...]
        n_sc[half:, :] = n1_ref[...]
        lab_sc[...] = columns(lab_ref[...])
        m_sc[...] = jnp.full(m_sc.shape, -jnp.inf, F32)
        s_sc[...] = jnp.zeros(s_sc.shape, F32)
        t_sc[...] = jnp.zeros(t_sc.shape, F32)

    for c in range(0, tile, chunk):
        z = jnp.dot(n_sc[...], w_ref[:, c:c + chunk], preferred_element_type=F32)
        z_ref[:, c:c + chunk] = z
        lab = lab_sc[:, 0:1].astype(I32) - (j * tile + c)
        parts = []
        for k in range(0, chunk, LANES):
            zk = z[:, k:k + LANES]
            hot = lax.broadcasted_iota(I32, zk.shape, 1) + k == lab
            if c + k >= vocab % tile:
                inside = j * tile + c + k < vocab
                hot = hot & inside
                zk = jnp.where(inside, zk, -jnp.inf)
            t_sc[...] += jnp.where(hot, zk, 0.0)
            parts.append(zk)
        old = m_sc[...]
        top = functools.reduce(jnp.maximum, parts, old)
        s_sc[...] = functools.reduce(jnp.add, [jnp.exp(zk - top) for zk in parts], s_sc[...] * jnp.exp(old - top))
        m_sc[...] = top

    @pl.when(j == pl.num_programs(0) - 1)
    def _():
        m = jnp.max(m_sc[...], axis=1, keepdims=True)
        s = jnp.sum(s_sc[...] * jnp.exp(m_sc[...] - m), axis=1, keepdims=True)
        t = jnp.sum(t_sc[...], axis=1, keepdims=True)
        lane = lax.broadcasted_iota(I32, (m.shape[0], LANES), 1)
        st_ref[...] = jnp.transpose(jnp.where(lane == 0, m, jnp.where(lane == 1, s, t)))[:ROWS, :]


def own_logits(n0, n1, w, lab, tile=768, chunk=256):
    half, h = n0.shape
    t, v = 2 * half, w.shape[1]
    return call(
        functools.partial(own_body, tile=tile, chunk=chunk, vocab=v),
        grid=(pl.cdiv(v, tile),),
        in_specs=[whole((half, h)), whole((half, h)), pl.BlockSpec((h, tile), lambda j: (0, j)), whole((ROWS, t))],
        out_specs=[pl.BlockSpec((t, tile), lambda j: (0, j)), whole((ROWS, t))],
        out_shape=[jax.ShapeDtypeStruct((t, v), F32), jax.ShapeDtypeStruct((ROWS, t), F32)],
        scratch_shapes=[pltpu.VMEM((t, h), BF16)] + [pltpu.VMEM((t, LANES), F32)] * 4,
        cost=(2 * t * h * v, 2 * h * v + 4 * t * v),
    )(n0, n1, w, lab)


def combine_body(tp_ref, mine_ref, other_ref, info_ref, aux_ref):
    first = tp_ref[0] == 0
    mine, other, info = mine_ref[...], other_ref[...], info_ref[...]
    a, b = jnp.where(first, mine, other), jnp.where(first, other, mine)
    top = jnp.maximum(a[0:1], b[0:1])
    log_z = top + jnp.log(a[1:2] * jnp.exp(a[0:1] - top) + b[1:2] * jnp.exp(b[0:1] - top))
    mask, label, count = info[1:2], info[0:1], info[2:3]
    lost = jnp.sum(mask * (log_z - (a[2:3] + b[2:3])), axis=1, keepdims=True)
    row = lax.broadcasted_iota(I32, aux_ref.shape, 0)
    out = jnp.where(row == 0, log_z, jnp.where(row == 1, mask, jnp.where(row == 2, label, jnp.where(row == 3, count, lost))))
    aux_ref[...] = out


def combine(tp, mine, other, info):
    shape = mine.shape
    return call(
        combine_body,
        in_specs=[pl.BlockSpec(memory_space=pltpu.SMEM)] + [whole(shape)] * 3,
        out_specs=whole(shape),
        out_shape=jax.ShapeDtypeStruct(shape, F32),
        cost=(1000, 1000),
    )(tp, mine, other, info)


def back_body(z_ref, w_ref, own_ref, ax_ref, ay_ref, ad_ref, g_ref, dn_ref, cols, *, tile, vocab, rows):
    j = pl.program_id(0)
    last = pl.num_programs(0) - 1

    @pl.when(j == 0)
    def _():
        cols[...] = token_columns(own_ref[...], own_ref, ax_ref, ay_ref, ad_ref)
        dn_ref[...] = jnp.zeros(dn_ref.shape, F32)

    def step(width):
        g = softmax_grad(z_ref[:, :width], cols, j * tile)
        g_ref[:, :width] = g
        for c in range(0, w_ref.shape[0], rows):
            dn_ref[:, c:c + rows] += lax.dot_general(g, w_ref[c:c + rows, :width], NT, preferred_element_type=F32)

    @pl.when(j < last)
    def _():
        step(tile)

    @pl.when(j == last)
    def _():
        step(vocab - (pl.cdiv(vocab, tile) - 1) * tile)


def own_grad(z, w, auxes, slots, tile=1024, rows=1024):
    t, v = z.shape
    h = w.shape[0]
    return call(
        functools.partial(back_body, tile=tile, vocab=v, rows=rows),
        grid=(pl.cdiv(v, tile),),
        in_specs=[pl.BlockSpec((t, tile), lambda j: (0, j)), pl.BlockSpec((h, tile), lambda j: (0, j))] + [whole((ROWS, t))] * 4,
        out_specs=[pl.BlockSpec((t, tile), lambda j: (0, j)), whole((t, h))],
        out_shape=[jax.ShapeDtypeStruct((slots * t, v), BF16), jax.ShapeDtypeStruct((t, h), F32)],
        scratch_shapes=[pltpu.VMEM((t, LANES), F32)],
        cost=(2 * t * h * v, 2 * h * v + 6 * t * v),
    )(z, w, *auxes)


def remote_body(h0_ref, h1_ref, gain_ref, w_ref, own_ref, ax_ref, ay_ref, ad_ref, _, g_ref, n_ref, cols, *, tile, chunk, pick):
    half = h0_ref.shape[0]

    @pl.when(pl.program_id(0) == 0)
    def _():
        n_ref[:half, :] = (h0_ref[...] * gain_ref[...]).astype(BF16)
        n_ref[half:, :] = (h1_ref[...] * gain_ref[...]).astype(BF16)
        from_other = (ax_ref, ay_ref, ad_ref)
        lane = lax.broadcasted_iota(I32, ax_ref.shape, 1)
        (a, a_half), (b, _) = pick
        picked = jnp.where((lane < half) == (a_half == 0), from_other[a][...], from_other[b][...])
        if a_half != 0:
            picked = pltpu.roll(picked, half, 1)
        cols[...] = token_columns(picked, own_ref, ax_ref, ay_ref, ad_ref)

    for c in range(0, tile, chunk):
        z = jnp.dot(n_ref[...], w_ref[:, c:c + chunk], preferred_element_type=F32)
        g_ref[:, c:c + chunk] = softmax_grad(z, cols, pl.program_id(0) * tile + c)


def remote_grad(h0, h1, gain, w, auxes, g_all, slot, pick, tile=768, chunk=256):
    half, h = h0.shape
    t, v = 2 * half, w.shape[1]
    return call(
        functools.partial(remote_body, tile=tile, chunk=chunk, pick=pick),
        grid=(pl.cdiv(v, tile),),
        in_specs=[whole((half, h)), whole((half, h)), whole((1, h)), pl.BlockSpec((h, tile), lambda j: (0, j))] + [whole((ROWS, t))] * 4 + [pl.BlockSpec(memory_space=pl.ANY)],
        out_specs=[pl.BlockSpec((t, tile), lambda j: (slot, j)), whole((t, h))],
        out_shape=[jax.ShapeDtypeStruct(g_all.shape, BF16), jax.ShapeDtypeStruct((t, h), BF16)],
        scratch_shapes=[pltpu.VMEM((t, LANES), F32)],
        input_output_aliases={8: 0},
        cost=(2 * t * h * v, 2 * h * v + 2 * t * v),
    )(h0, h1, gain, w, *auxes, g_all)


def wgrad_body(at_ref, *refs, tile, chunk, pieces, with_add):
    n_refs, g_ref, rest, nt = refs[:pieces], refs[pieces], refs[pieces + 1:-1], refs[-1]
    out_ref = rest[-1]

    @pl.when(pl.program_id(0) == 0)
    def _():
        first = 0
        for ref in n_refs:
            size = ref.shape[0]
            nt[:, first:first + size] = jnp.transpose(ref[...].astype(F32)).astype(BF16)
            first += size

    for c in range(0, tile, chunk):
        part = jnp.dot(nt[...], g_ref[:, c:c + chunk], preferred_element_type=F32)
        out_ref[:, c:c + chunk] = part + rest[0][:, c:c + chunk] if with_add else part


def weight_grad(at, ns, g, first, tiles, add=None, into=None, tile=1792, chunk=256):
    k, v = g.shape
    r = k // 4
    width = min(v - first * tile, tiles * tile)
    ins, aliases = [*ns, g], {}
    specs = [pl.BlockSpec((n.shape[0], r), lambda j, at_ref: (0, at_ref[0])) for n in ns] + [pl.BlockSpec((k, tile), lambda j, at_ref: (0, j + first))]
    out_spec, out_shape = pl.BlockSpec((r, tile), lambda j, at_ref: (0, j)), (r, width)
    if add is not None:
        ins.append(add)
        specs.append(pl.BlockSpec((r, tile), lambda j, at_ref: (0, j)))
        out_spec, out_shape = pl.BlockSpec((r, tile), lambda j, at_ref: (0, j + first)), (r, v)
        if into is not None:
            ins.append(into)
            specs.append(pl.BlockSpec(memory_space=pl.ANY))
            aliases = {len(ins): 0}
    return call(
        functools.partial(wgrad_body, tile=tile, chunk=chunk, pieces=len(ns), with_add=add is not None),
        grid_spec=pltpu.PrefetchScalarGridSpec(num_scalar_prefetch=1, grid=(tiles,), in_specs=specs, out_specs=out_spec, scratch_shapes=[pltpu.VMEM((r, k), BF16)]),
        out_shape=jax.ShapeDtypeStruct(out_shape, F32),
        input_output_aliases=aliases,
        cost=(2 * r * k * width, 2 * k * width + 4 * r * width),
    )(at, *ins)


def final_body(x_ref, inv0_ref, inv1_ref, gain_ref, mine_ref, other_ref, dh_ref, gam_ref):
    j = pl.program_id(0)
    first = j < pl.num_programs(0) // 2
    inv = jnp.where(first, inv0_ref[...], inv1_ref[...])
    hat = x_ref[...].astype(F32) * inv
    dn = mine_ref[...] + other_ref[...]
    prod = dn * hat

    @pl.when(j == 0)
    def _():
        gam_ref[...] = jnp.zeros(gam_ref.shape, F32)

    gam_ref[...] += jnp.sum(prod.reshape(-1, ROWS, prod.shape[1]), axis=0)
    d_hat = dn * gain_ref[...]
    dh_ref[...] = (inv * (d_hat - hat * jnp.mean(d_hat * hat, axis=-1, keepdims=True))).astype(BF16)


def final(x, inv0, inv1, gain, mine, other, block=64):
    t, h = x.shape
    steps = t // block
    half = steps // 2
    rows = pl.BlockSpec((block, h), lambda j: (j, 0))
    return call(
        final_body,
        grid=(steps,),
        in_specs=[rows, pl.BlockSpec((block, 1), lambda j: (jnp.minimum(j, half - 1), 0)), pl.BlockSpec((block, 1), lambda j: (jnp.maximum(j - half, 0), 0)), whole((1, h)), rows, rows],
        out_specs=[rows, whole((ROWS, h))],
        out_shape=[jax.ShapeDtypeStruct((t, h), BF16), jax.ShapeDtypeStruct((ROWS, h), F32)],
        cost=(10 * t * h, 12 * t * h),
    )(x, inv0, inv1, gain, mine, other)


def solution(mesh):
    n_dp = mesh.shape["dp"]

    def swap(v, bits):
        return lax.ppermute(v, "dp", [(i, i ^ bits) for i in range(n_dp)])

    def swap_tp(v):
        return lax.ppermute(v, "tp", [(0, 1), (1, 0)])

    def step(hidden_in, labels, loss_mask, norm_gamma, w_local):
        tp, dp = lax.axis_index("tp"), lax.axis_index("dp")
        gain = norm_gamma.astype(F32)[None, :]
        mask = loss_mask.astype(F32)
        count = jnp.sum(mask).reshape(1, 1)
        count = count + swap(count, 1)
        local = (labels - tp * w_local.shape[1]).astype(F32)
        info = jnp.concatenate([local[None], mask[None], jnp.broadcast_to(count, (ROWS - 2, mask.shape[0]))], axis=0)

        low, n_low, inv_low = prep_half(hidden_in, gain, 0)
        high, n_high, inv_high = prep_half(hidden_in, gain, 1)
        x_low, y_high = swap(low, 2), swap(high, 4)
        lab_rows = jnp.broadcast_to(local[None], (ROWS, mask.shape[0]))
        logits, stats = own_logits(n_low, n_high, w_local, lab_rows)
        aux = combine(tp.reshape(1), stats, swap_tp(stats), info)
        aux_x, aux_y, aux_d = swap(aux, 2), swap(aux, 4), swap(aux, 6)
        auxes = (aux, aux_x, aux_y, aux_d)
        x_low, y_high, low, high, auxes = lax.optimization_barrier((x_low, y_high, low, high, auxes))
        d_low, d_high = swap(x_low, 4), swap(y_high, 2)
        x_high, y_low = swap(high, 2), swap(low, 4)

        g_all, dn_mine = own_grad(logits, w_local, auxes, 4)
        dn_other = swap_tp(dn_mine)
        ns = [n_low, n_high]
        for slot, h0, h1, pick in ((1, x_low, y_high, ((0, 0), (1, 1))), (2, d_low, d_high, ((2, 0), (2, 1))), (3, x_high, y_low, ((0, 1), (1, 0)))):
            g_all, n = remote_grad(h0, h1, gain, w_local, auxes, g_all, slot, pick)
            ns.append(n)

        own_at, other_at = dp.reshape(1), (dp ^ 1).reshape(1)
        p1 = swap(weight_grad(other_at, ns, g_all, 0, 5), 1)
        p2 = swap(weight_grad(other_at, ns, g_all, 5, 4), 1)
        d_w_out = weight_grad(own_at, ns, g_all, 0, 5, add=p1)
        d_w_out = weight_grad(own_at, ns, g_all, 5, 4, add=p2, into=d_w_out)

        d_hidden, gam = final(hidden_in, inv_low, inv_high, gain, dn_mine, dn_other)
        d_gamma = jnp.sum(gam, axis=0)
        for bit in (1, 2, 4):
            d_gamma = d_gamma + swap(d_gamma, bit)
        total = (aux[3, 0] + aux_x[3, 0]) + (aux_y[3, 0] + aux_d[3, 0])
        lost = ((aux[4, 0] + aux_x[4, 0]) + (aux_y[4, 0] + aux_d[4, 0])).reshape(1)
        loss = (lost + swap(lost, 1))[0] / total
        return (loss, d_hidden, d_w_out, d_gamma)

    return jax.shard_map(step, mesh=mesh, in_specs=(P("dp", None), P("dp"), P("dp"), P(), P(None, "tp")), out_specs=(P(), P("dp", None), P("dp", "tp"), P()), check_vma=False)
```

```python
import functools

import jax
import jax.numpy as jnp
from jax import lax
from jax.experimental import pallas as pl
from jax.experimental.pallas import tpu as pltpu
from jax.sharding import PartitionSpec as P

NORM_EPS = 1e-5
F32, BF16, I32 = jnp.float32, jnp.bfloat16, jnp.int32
VMEM_LIMIT = 64 * 1024 * 1024 - 64 * 1024
LANES = 128
ROWS = 8
NT = (((1,), (1,)), ((), ()))


def call(body, **kw):
    cost = kw.pop("cost")
    return pl.pallas_call(body, compiler_params=pltpu.CompilerParams(vmem_limit_bytes=VMEM_LIMIT), cost_estimate=pl.CostEstimate(flops=cost[0], bytes_accessed=cost[1], transcendentals=0), **kw)


def whole(shape):
    return pl.BlockSpec(shape, lambda *_: (0,) * len(shape))


def columns(rows):
    return jnp.transpose(jnp.concatenate([rows] * (LANES // ROWS), axis=0))


def softmax_grad(z, cols, first):
    hot = lax.broadcasted_iota(I32, z.shape, 1) + first == cols[:, 2:3].astype(I32)
    return ((jnp.exp(z - cols[:, 0:1]) - hot.astype(F32)) * cols[:, 1:2]).astype(BF16)


def token_columns(picked, aux_own, aux_x, aux_y, aux_d):
    count = aux_own[3:4, 0:1] + aux_x[3:4, 0:1] + aux_y[3:4, 0:1] + aux_d[3:4, 0:1]
    row = lax.broadcasted_iota(I32, picked.shape, 0)
    return columns(jnp.where(row == 1, picked / count, picked))


def prep_body(tp_ref, x_ref, gain_ref, lab_ref, mask_ref, low_ref, high_ref, n_ref, inv_ref, rows_ref, cnt_ref, *, vocab):
    j = pl.program_id(0)
    half = pl.num_programs(0) // 2
    x = x_ref[...].astype(F32)
    inv = lax.rsqrt(jnp.mean(x * x, axis=-1, keepdims=True) + NORM_EPS)
    hat = x * inv
    n_ref[...] = (hat * gain_ref[...].astype(F32)).astype(BF16)
    inv_ref[...] = inv

    @pl.when(j < half)
    def _():
        low_ref[...] = hat

    @pl.when(j >= half)
    def _():
        high_ref[...] = hat

    @pl.when(j == 0)
    def _():
        mask = mask_ref[...].astype(F32)
        label = (lab_ref[...] - tp_ref[0] * vocab).astype(F32)
        row = lax.broadcasted_iota(I32, rows_ref.shape, 0)
        rows_ref[...] = jnp.where(row == 0, label, mask)
        cnt_ref[...] = jnp.broadcast_to(jnp.sum(mask, axis=1, keepdims=True), cnt_ref.shape)


def prep(tp, x, gain, labels, mask, vocab, block=128):
    t, h = x.shape
    steps = t // block
    half = steps // 2
    rows = pl.BlockSpec((block, h), lambda j: (j, 0))
    return call(
        functools.partial(prep_body, vocab=vocab),
        grid=(steps,),
        in_specs=[pl.BlockSpec(memory_space=pltpu.SMEM), rows, whole((1, h)), whole((1, t)), whole((1, t))],
        out_specs=[
            pl.BlockSpec((block, h), lambda j: (jnp.minimum(j, half - 1), 0)), pl.BlockSpec((block, h), lambda j: (jnp.maximum(j - half, 0), 0)),
            rows, pl.BlockSpec((block, 1), lambda j: (j, 0)), whole((ROWS, t)), whole((ROWS, LANES)),
        ],
        out_shape=[
            jax.ShapeDtypeStruct((t // 2, h), F32), jax.ShapeDtypeStruct((t // 2, h), F32), jax.ShapeDtypeStruct((t, h), BF16),
            jax.ShapeDtypeStruct((t, 1), F32), jax.ShapeDtypeStruct((ROWS, t), F32), jax.ShapeDtypeStruct((ROWS, LANES), F32),
        ],
        cost=(8 * t * h, 8 * t * h),
    )(tp, x, gain, labels, mask)


def own_body(n_ref, w_ref, rows_ref, z_ref, st_ref, lab_sc, m_sc, s_sc, t_sc, *, tile, block, vocab):
    j = pl.program_id(0)

    @pl.when(j == 0)
    def _():
        lab_sc[...] = columns(rows_ref[...])
        m_sc[...] = jnp.full(m_sc.shape, -jnp.inf, F32)
        s_sc[...] = jnp.zeros(s_sc.shape, F32)
        t_sc[...] = jnp.zeros(t_sc.shape, F32)

    for r in range(0, n_ref.shape[0], block):
        at = slice(r, r + block)
        z = jnp.dot(n_ref[at, :], w_ref[...], preferred_element_type=F32)
        z_ref[at, :] = z
        lab = lab_sc[at, 0:1].astype(I32) - j * tile
        parts, targets = [], []
        for k in range(0, tile, LANES):
            zk = z[:, k:k + LANES]
            hot = lax.broadcasted_iota(I32, zk.shape, 1) + k == lab
            if k >= vocab % tile:
                inside = j * tile + k < vocab
                hot = hot & inside
                zk = jnp.where(inside, zk, -jnp.inf)
            targets.append(jnp.where(hot, zk, 0.0))
            parts.append(zk)
        t_sc[at, :] += functools.reduce(jnp.add, targets)
        old = m_sc[at, :]
        top = functools.reduce(jnp.maximum, parts, old)
        s_sc[at, :] = functools.reduce(jnp.add, [jnp.exp(zk - top) for zk in parts], s_sc[at, :] * jnp.exp(old - top))
        m_sc[at, :] = top

    @pl.when(j == pl.num_programs(0) - 1)
    def _():
        m = jnp.max(m_sc[...], axis=1, keepdims=True)
        s = jnp.sum(s_sc[...] * jnp.exp(m_sc[...] - m), axis=1, keepdims=True)
        t = jnp.sum(t_sc[...], axis=1, keepdims=True)
        lane = lax.broadcasted_iota(I32, (m.shape[0], LANES), 1)
        st_ref[...] = jnp.transpose(jnp.where(lane == 0, m, jnp.where(lane == 1, s, t)))[:ROWS, :]


def own_logits(n, w, rows, tile=768, block=128):
    t, h = n.shape
    v = w.shape[1]
    return call(
        functools.partial(own_body, tile=tile, block=block, vocab=v),
        grid=(pl.cdiv(v, tile),),
        in_specs=[whole((t, h)), pl.BlockSpec((h, tile), lambda j: (0, j)), whole((ROWS, t))],
        out_specs=[pl.BlockSpec((t, tile), lambda j: (0, j)), whole((ROWS, t))],
        out_shape=[jax.ShapeDtypeStruct((t, v), F32), jax.ShapeDtypeStruct((ROWS, t), F32)],
        scratch_shapes=[pltpu.VMEM((t, LANES), F32)] * 4,
        cost=(2 * t * h * v, 2 * h * v + 4 * t * v),
    )(n, w, rows)


def combine_body(tp_ref, mine_ref, other_ref, rows_ref, cnt0_ref, cnt1_ref, aux_ref):
    first = tp_ref[0] == 0
    mine, other = mine_ref[...], other_ref[...]
    label, mask = rows_ref[0:1, :], rows_ref[1:2, :]
    a, b = jnp.where(first, mine, other), jnp.where(first, other, mine)
    top = jnp.maximum(a[0:1], b[0:1])
    log_z = top + jnp.log(a[1:2] * jnp.exp(a[0:1] - top) + b[1:2] * jnp.exp(b[0:1] - top))
    count = cnt0_ref[0:1, 0:1] + cnt1_ref[0:1, 0:1]
    lost = jnp.sum(mask * (log_z - (a[2:3] + b[2:3])), axis=1, keepdims=True)
    row = lax.broadcasted_iota(I32, aux_ref.shape, 0)
    aux_ref[...] = jnp.where(row == 0, log_z, jnp.where(row == 1, mask, jnp.where(row == 2, label, jnp.where(row == 3, count, lost))))


def combine(tp, mine, other, rows, cnt0, cnt1):
    return call(
        combine_body,
        in_specs=[pl.BlockSpec(memory_space=pltpu.SMEM)] + [whole(mine.shape)] * 3 + [whole(cnt0.shape)] * 2,
        out_specs=whole(mine.shape),
        out_shape=jax.ShapeDtypeStruct(mine.shape, F32),
        cost=(1000, 1000),
    )(tp, mine, other, rows, cnt0, cnt1)


def back_body(z_ref, w_ref, own_ref, ax_ref, ay_ref, ad_ref, g_ref, dn_ref, sum_ref, cols, *, tile, vocab, rows):
    j = pl.program_id(0)

    @pl.when(j == 0)
    def _():
        cols[...] = token_columns(own_ref[...], own_ref, ax_ref, ay_ref, ad_ref)
        dn_ref[...] = jnp.zeros(dn_ref.shape, F32)
        sums = (own_ref[...] + ax_ref[...]) + (ay_ref[...] + ad_ref[...])
        row = lax.broadcasted_iota(I32, sum_ref.shape, 0)
        sum_ref[...] = jnp.where(row == 0, sums[4:5, 0:1], sums[3:4, 0:1])

    @pl.when(j == pl.num_programs(0) - 1)
    def _():
        width = vocab - (pl.cdiv(vocab, tile) - 1) * tile
        z_ref[:, width:] = jnp.zeros((z_ref.shape[0], tile - width), F32)
        w_ref[:, width:] = jnp.zeros((w_ref.shape[0], tile - width), BF16)

    g_ref[...] = softmax_grad(z_ref[...], cols, j * tile)
    for c in range(0, w_ref.shape[0], rows):
        dn_ref[:, c:c + rows] += lax.dot_general(g_ref[...], w_ref[c:c + rows, :], NT, preferred_element_type=F32)


def own_grad(z, w, auxes, slots, tile=1024, rows=1024):
    t, v = z.shape
    h = w.shape[0]
    return call(
        functools.partial(back_body, tile=tile, vocab=v, rows=rows),
        grid=(pl.cdiv(v, tile),),
        in_specs=[pl.BlockSpec((t, tile), lambda j: (0, j)), pl.BlockSpec((h, tile), lambda j: (0, j))] + [whole((ROWS, t))] * 4,
        out_specs=[pl.BlockSpec((t, tile), lambda j: (0, j)), whole((t, h)), whole((ROWS, LANES))],
        out_shape=[jax.ShapeDtypeStruct((slots * t, v), BF16), jax.ShapeDtypeStruct((t, h), F32), jax.ShapeDtypeStruct((ROWS, LANES), F32)],
        scratch_shapes=[pltpu.VMEM((t, LANES), F32)],
        cost=(2 * t * h * v, 2 * h * v + 6 * t * v),
    )(z, w, *auxes)


def remote_body(slot_ref, h0_ref, h1_ref, gain_ref, w_ref, own_ref, ax_ref, ay_ref, ad_ref, _, g_ref, n_ref, cols, *, tile, chunk):
    half = h0_ref.shape[0]

    @pl.when(pl.program_id(0) == 0)
    def _():
        n_ref[:half, :] = (h0_ref[...] * gain_ref[...].astype(F32)).astype(BF16)
        n_ref[half:, :] = (h1_ref[...] * gain_ref[...].astype(F32)).astype(BF16)
        first = lax.broadcasted_iota(I32, ax_ref.shape, 1) < half
        straight = jnp.where(first, ax_ref[...], ay_ref[...])
        crossed = pltpu.roll(jnp.where(first, ay_ref[...], ax_ref[...]), half, 1)
        picked = jnp.where(slot_ref[0] == 1, straight, jnp.where(slot_ref[0] == 2, ad_ref[...], crossed))
        cols[...] = token_columns(picked, own_ref, ax_ref, ay_ref, ad_ref)

    for c in range(0, tile, chunk):
        z = jnp.dot(n_ref[...], w_ref[:, c:c + chunk], preferred_element_type=F32)
        g_ref[:, c:c + chunk] = softmax_grad(z, cols, pl.program_id(0) * tile + c)


def remote_grad(slot, h0, h1, gain, w, auxes, g_all, tile=768, chunk=256):
    half, h = h0.shape
    t, v = 2 * half, w.shape[1]
    return call(
        functools.partial(remote_body, tile=tile, chunk=chunk),
        grid_spec=pltpu.PrefetchScalarGridSpec(
            num_scalar_prefetch=1, grid=(pl.cdiv(v, tile),),
            in_specs=[whole((half, h)), whole((half, h)), whole((1, h)), pl.BlockSpec((h, tile), lambda j, slot_ref: (0, j))] + [whole((ROWS, t))] * 4 + [pl.BlockSpec(memory_space=pl.ANY)],
            out_specs=[pl.BlockSpec((t, tile), lambda j, slot_ref: (slot_ref[0], j)), whole((t, h))],
            scratch_shapes=[pltpu.VMEM((t, LANES), F32)],
        ),
        out_shape=[jax.ShapeDtypeStruct(g_all.shape, BF16), jax.ShapeDtypeStruct((t, h), BF16)],
        input_output_aliases={9: 0},
        cost=(2 * t * h * v, 2 * h * v + 2 * t * v),
    )(slot, h0, h1, gain, w, *auxes, g_all)


def wgrad_first_body(at_ref, *refs, tile, chunk, pieces):
    g_ref, out_ref, nts = refs[2 * pieces], refs[-3], refs[-2:]

    @pl.when(pl.program_id(0) == 0)
    def _():
        for k in range(2):
            first = 0
            for ref in refs[k * pieces:(k + 1) * pieces]:
                size = ref.shape[0]
                nts[k][:, first:first + size] = jnp.transpose(ref[...].astype(F32)).astype(BF16)
                first += size

    for c in range(0, tile, chunk):
        out_ref[:, c:c + chunk] = jnp.dot(nts[0][...], g_ref[:, c:c + chunk], preferred_element_type=F32)


def weight_grad_first(at, ns, g, tiles, tile=1792, chunk=256):
    k, _ = g.shape
    r = k // 4
    width = tiles * tile
    states = [pl.BlockSpec((n.shape[0], r), functools.partial(lambda which, j, at_ref: (0, at_ref[which]), which)) for which in range(2) for n in ns]
    return call(
        functools.partial(wgrad_first_body, tile=tile, chunk=chunk, pieces=len(ns)),
        grid_spec=pltpu.PrefetchScalarGridSpec(
            num_scalar_prefetch=1, grid=(tiles,), in_specs=states + [pl.BlockSpec((k, tile), lambda j, at_ref: (0, j))],
            out_specs=[pl.BlockSpec((r, tile), lambda j, at_ref: (0, j)), whole((r, k)), whole((r, k))],
        ),
        out_shape=[jax.ShapeDtypeStruct((r, width), F32)] + [jax.ShapeDtypeStruct((r, k), BF16)] * 2,
        cost=(2 * r * k * width, 2 * k * width + 4 * r * width),
    )(at, *ns, *ns, g)


def wgrad_body(nt_ref, g_ref, *rest, tile, chunk, with_add, with_sums):
    out_ref = rest[-3] if with_sums else rest[-1]
    if with_sums:
        gams, (sum0_ref, sum1_ref), (gam_ref, loss_ref) = rest[1:5], rest[5:7], rest[-2:]

        @pl.when(pl.program_id(0) == 0)
        def _():
            gam_ref[...] = (gams[0][...] + gams[1][...]) + (gams[2][...] + gams[3][...])
            loss_ref[...] = jnp.broadcast_to((sum0_ref[0:1, :] + sum1_ref[0:1, :]) / sum0_ref[1:2, :], loss_ref.shape)

    for c in range(0, tile, chunk):
        part = jnp.dot(nt_ref[...], g_ref[:, c:c + chunk], preferred_element_type=F32)
        out_ref[:, c:c + chunk] = part + rest[0][:, c:c + chunk] if with_add else part


def weight_grad(nt, g, first, tiles, add=None, into=None, sums=None, tile=1792, chunk=256):
    r, k = nt.shape
    v = g.shape[1]
    width = min(v - first * tile, tiles * tile)
    ins, aliases = [nt, g], {}
    specs = [whole((r, k)), pl.BlockSpec((k, tile), lambda j: (0, j + first))]
    out_specs, out_shape = pl.BlockSpec((r, tile), lambda j: (0, j)), jax.ShapeDtypeStruct((r, width), F32)
    if add is not None:
        ins.append(add)
        specs.append(pl.BlockSpec((r, tile), lambda j: (0, j)))
        out_specs, out_shape = pl.BlockSpec((r, tile), lambda j: (0, j + first)), jax.ShapeDtypeStruct((r, v), F32)
    if into is not None:
        aliases = {len(ins): 0}
        ins.append(into)
        specs.append(pl.BlockSpec(memory_space=pl.ANY))
    if sums is not None:
        ins.extend(sums)
        specs.extend(whole(a.shape) for a in sums)
        out_specs = [out_specs, whole(sums[0].shape), whole(sums[-1].shape)]
        out_shape = [out_shape, jax.ShapeDtypeStruct(sums[0].shape, F32), jax.ShapeDtypeStruct(sums[-1].shape, F32)]
    return call(
        functools.partial(wgrad_body, tile=tile, chunk=chunk, with_add=add is not None, with_sums=sums is not None),
        grid=(tiles,),
        in_specs=specs,
        out_specs=out_specs,
        out_shape=out_shape,
        input_output_aliases=aliases,
        cost=(2 * r * k * width, 2 * k * width + 4 * r * width),
    )(*ins)


def final_body(x_ref, inv_ref, gain_ref, mine_ref, other_ref, dh_ref, gam_ref):
    inv = inv_ref[...]
    hat = x_ref[...].astype(F32) * inv
    dn = mine_ref[...] + other_ref[...]
    prod = dn * hat

    @pl.when(pl.program_id(0) == 0)
    def _():
        gam_ref[...] = jnp.zeros(gam_ref.shape, F32)

    gam_ref[...] += jnp.sum(prod.reshape(-1, ROWS, prod.shape[1]), axis=0)
    d_hat = dn * gain_ref[...].astype(F32)
    dh_ref[...] = (inv * (d_hat - hat * jnp.mean(d_hat * hat, axis=-1, keepdims=True))).astype(BF16)


def final(x, inv, gain, mine, other, block=64):
    t, h = x.shape
    rows = pl.BlockSpec((block, h), lambda j: (j, 0))
    return call(
        final_body,
        grid=(t // block,),
        in_specs=[rows, pl.BlockSpec((block, 1), lambda j: (j, 0)), whole((1, h)), rows, rows],
        out_specs=[rows, whole((ROWS, h))],
        out_shape=[jax.ShapeDtypeStruct((t, h), BF16), jax.ShapeDtypeStruct((ROWS, h), F32)],
        cost=(10 * t * h, 12 * t * h),
    )(x, inv, gain, mine, other)


def solution(mesh):
    n_dp = mesh.shape["dp"]

    def swap(v, bits):
        return lax.ppermute(v, "dp", [(i, i ^ bits) for i in range(n_dp)])

    def swap_tp(v):
        return lax.ppermute(v, "tp", [(0, 1), (1, 0)])

    def step(hidden_in, labels, loss_mask, norm_gamma, w_local):
        tp, dp = lax.axis_index("tp").reshape(1), lax.axis_index("dp").reshape(1)
        gain = norm_gamma[None, :]
        low, high, n_own, inv, rows, cnt = prep(tp, hidden_in, gain, labels[None], loss_mask[None], w_local.shape[1])
        cnt_other = swap(cnt, 1)
        x_low, y_high = swap(low, 2), swap(high, 4)
        logits, stats = own_logits(n_own, w_local, rows)
        aux = combine(tp, stats, swap_tp(stats), rows, cnt, cnt_other)
        aux_x, aux_y, aux_d = swap(aux, 2), swap(aux, 4), swap(aux, 6)
        auxes = (aux, aux_x, aux_y, aux_d)
        x_low, y_high, low, high, auxes = lax.optimization_barrier((x_low, y_high, low, high, auxes))
        d_low, d_high = swap(x_low, 4), swap(y_high, 2)
        x_high, y_low = swap(high, 2), swap(low, 4)

        g_all, dn_mine, sums = own_grad(logits, w_local, auxes, 4)
        dn_other = swap_tp(dn_mine)
        sums_other = swap(sums, 1)
        ns = [n_own]
        for slot, h0, h1 in ((1, x_low, y_high), (2, d_low, d_high), (3, x_high, y_low)):
            g_all, n = remote_grad(jnp.array([slot], I32), h0, h1, gain, w_local, auxes, g_all)
            ns.append(n)

        at = jnp.concatenate([dp ^ 1, dp])
        p1, nt_other, nt_own = weight_grad_first(at, ns, g_all, 5)
        p1 = swap(p1, 1)
        p2 = swap(weight_grad(nt_other, g_all, 5, 4), 1)
        d_hidden, gam = final(hidden_in, inv, gain, dn_mine, dn_other)
        sums = (gam, swap(gam, 2), swap(gam, 4), swap(gam, 6), sums, sums_other)
        d_w_out, gam, loss = weight_grad(nt_own, g_all, 0, 5, add=p1, sums=sums)
        d_w_out = weight_grad(nt_own, g_all, 5, 4, add=p2, into=d_w_out)
        d_gamma = jnp.sum(gam + swap(gam, 1), axis=0)
        loss = loss[0, 0]
        return (loss, d_hidden, d_w_out, d_gamma)

    return jax.shard_map(step, mesh=mesh, in_specs=(P("dp", None), P("dp"), P("dp"), P(), P(None, "tp")), out_specs=(P(), P("dp", None), P("dp", "tp"), P()), check_vma=False)
```

```python
import functools

import jax
import jax.numpy as jnp
from jax import lax
from jax.experimental import pallas as pl
from jax.experimental.pallas import tpu as pltpu
from jax.sharding import PartitionSpec as P

NORM_EPS = 1e-5
F32, BF16, I32 = jnp.float32, jnp.bfloat16, jnp.int32
VMEM_LIMIT = 64 * 1024 * 1024 - 64 * 1024
LANES = 128
ROWS = 8
HEAD = 10240
NT = (((1,), (1,)), ((), ()))


def call(body, **kw):
    cost = kw.pop("cost")
    return pl.pallas_call(body, compiler_params=pltpu.CompilerParams(vmem_limit_bytes=VMEM_LIMIT), cost_estimate=pl.CostEstimate(flops=cost[0], bytes_accessed=cost[1], transcendentals=0), **kw)


def whole(shape):
    return pl.BlockSpec(shape, lambda *_: (0,) * len(shape))


def columns(rows):
    return jnp.transpose(jnp.concatenate([rows] * (LANES // ROWS), axis=0))


def softmax_grad(z, cols, first):
    hot = lax.broadcasted_iota(I32, z.shape, 1) + first == cols[:, 2:3].astype(I32)
    return ((jnp.exp(z - cols[:, 0:1]) - hot.astype(F32)) * cols[:, 1:2]).astype(BF16)


def token_columns(picked, aux_own, aux_x, aux_y, aux_d):
    count = aux_own[3:4, 0:1] + aux_x[3:4, 0:1] + aux_y[3:4, 0:1] + aux_d[3:4, 0:1]
    row = lax.broadcasted_iota(I32, picked.shape, 0)
    return columns(jnp.where(row == 1, picked / count, picked))


def prep_body(tp_ref, x_ref, gain_ref, lab_ref, mask_ref, low_ref, high_ref, n_ref, inv_ref, rows_ref, cnt_ref, *, vocab):
    j = pl.program_id(0)
    half = pl.num_programs(0) // 2
    x = x_ref[...].astype(F32)
    inv = lax.rsqrt(jnp.mean(x * x, axis=-1, keepdims=True) + NORM_EPS)
    hat = x * inv
    n_ref[...] = (hat * gain_ref[...].astype(F32)).astype(BF16)
    inv_ref[...] = inv

    @pl.when(j < half)
    def _():
        low_ref[...] = hat

    @pl.when(j >= half)
    def _():
        high_ref[...] = hat

    @pl.when(j == 0)
    def _():
        mask = mask_ref[...].astype(F32)
        label = (lab_ref[...] - tp_ref[0] * vocab).astype(F32)
        row = lax.broadcasted_iota(I32, rows_ref.shape, 0)
        rows_ref[...] = jnp.where(row == 0, label, mask)
        cnt_ref[...] = jnp.broadcast_to(jnp.sum(mask, axis=1, keepdims=True), cnt_ref.shape)


def prep(tp, x, gain, labels, mask, vocab, block=128):
    t, h = x.shape
    steps = t // block
    half = steps // 2
    rows = pl.BlockSpec((block, h), lambda j: (j, 0))
    return call(
        functools.partial(prep_body, vocab=vocab),
        grid=(steps,),
        in_specs=[pl.BlockSpec(memory_space=pltpu.SMEM), rows, whole((1, h)), whole((1, t)), whole((1, t))],
        out_specs=[
            pl.BlockSpec((block, h), lambda j: (jnp.minimum(j, half - 1), 0)), pl.BlockSpec((block, h), lambda j: (jnp.maximum(j - half, 0), 0)),
            rows, pl.BlockSpec((block, 1), lambda j: (j, 0)), whole((ROWS, t)), whole((ROWS, LANES)),
        ],
        out_shape=[
            jax.ShapeDtypeStruct((t // 2, h), F32), jax.ShapeDtypeStruct((t // 2, h), F32), jax.ShapeDtypeStruct((t, h), BF16),
            jax.ShapeDtypeStruct((t, 1), F32), jax.ShapeDtypeStruct((ROWS, t), F32), jax.ShapeDtypeStruct((ROWS, LANES), F32),
        ],
        cost=(8 * t * h, 8 * t * h),
    )(tp, x, gain, labels, mask)


def own_body(n_ref, w_ref, rows_ref, z_ref, st_ref, lab_sc, m_sc, s_sc, t_sc, *, tile, block, vocab):
    j = pl.program_id(0)

    @pl.when(j == 0)
    def _():
        lab_sc[...] = columns(rows_ref[...])
        m_sc[...] = jnp.full(m_sc.shape, -jnp.inf, F32)
        s_sc[...] = jnp.zeros(s_sc.shape, F32)
        t_sc[...] = jnp.zeros(t_sc.shape, F32)

    for r in range(0, n_ref.shape[0], block):
        at = slice(r, r + block)
        z = jnp.dot(n_ref[at, :], w_ref[...], preferred_element_type=F32)
        z_ref[at, :] = z
        lab = lab_sc[at, 0:1].astype(I32) - j * tile
        parts, targets = [], []
        for k in range(0, tile, LANES):
            zk = z[:, k:k + LANES]
            hot = lax.broadcasted_iota(I32, zk.shape, 1) + k == lab
            if k >= vocab % tile:
                inside = j * tile + k < vocab
                hot = hot & inside
                zk = jnp.where(inside, zk, -jnp.inf)
            targets.append(jnp.where(hot, zk, 0.0))
            parts.append(zk)
        t_sc[at, :] += functools.reduce(jnp.add, targets)
        old = m_sc[at, :]
        top = functools.reduce(jnp.maximum, parts, old)
        s_sc[at, :] = functools.reduce(jnp.add, [jnp.exp(zk - top) for zk in parts], s_sc[at, :] * jnp.exp(old - top))
        m_sc[at, :] = top

    @pl.when(j == pl.num_programs(0) - 1)
    def _():
        m = jnp.max(m_sc[...], axis=1, keepdims=True)
        s = jnp.sum(s_sc[...] * jnp.exp(m_sc[...] - m), axis=1, keepdims=True)
        t = jnp.sum(t_sc[...], axis=1, keepdims=True)
        lane = lax.broadcasted_iota(I32, (m.shape[0], LANES), 1)
        st_ref[...] = jnp.transpose(jnp.where(lane == 0, m, jnp.where(lane == 1, s, t)))[:ROWS, :]


def own_logits(n, w, rows, tile=768, block=128):
    t, h = n.shape
    v = w.shape[1]
    return call(
        functools.partial(own_body, tile=tile, block=block, vocab=v),
        grid=(pl.cdiv(v, tile),),
        in_specs=[whole((t, h)), pl.BlockSpec((h, tile), lambda j: (0, j)), whole((ROWS, t))],
        out_specs=[pl.BlockSpec((t, tile), lambda j: (0, j)), whole((ROWS, t))],
        out_shape=[jax.ShapeDtypeStruct((t, v), F32), jax.ShapeDtypeStruct((ROWS, t), F32)],
        scratch_shapes=[pltpu.VMEM((t, LANES), F32)] * 4,
        cost=(2 * t * h * v, 2 * h * v + 4 * t * v),
    )(n, w, rows)


def combine_body(tp_ref, mine_ref, other_ref, rows_ref, cnt0_ref, cnt1_ref, aux_ref):
    first = tp_ref[0] == 0
    mine, other = mine_ref[...], other_ref[...]
    label, mask = rows_ref[0:1, :], rows_ref[1:2, :]
    a, b = jnp.where(first, mine, other), jnp.where(first, other, mine)
    top = jnp.maximum(a[0:1], b[0:1])
    log_z = top + jnp.log(a[1:2] * jnp.exp(a[0:1] - top) + b[1:2] * jnp.exp(b[0:1] - top))
    count = cnt0_ref[0:1, 0:1] + cnt1_ref[0:1, 0:1]
    lost = jnp.sum(mask * (log_z - (a[2:3] + b[2:3])), axis=1, keepdims=True)
    row = lax.broadcasted_iota(I32, aux_ref.shape, 0)
    aux_ref[...] = jnp.where(row == 0, log_z, jnp.where(row == 1, mask, jnp.where(row == 2, label, jnp.where(row == 3, count, lost))))


def combine(tp, mine, other, rows, cnt0, cnt1):
    return call(
        combine_body,
        in_specs=[pl.BlockSpec(memory_space=pltpu.SMEM)] + [whole(mine.shape)] * 3 + [whole(cnt0.shape)] * 2,
        out_specs=whole(mine.shape),
        out_shape=jax.ShapeDtypeStruct(mine.shape, F32),
        cost=(1000, 1000),
    )(tp, mine, other, rows, cnt0, cnt1)


def back_body(z_ref, w_ref, own_ref, ax_ref, ay_ref, ad_ref, g_ref, dn_ref, sum_ref, low_ref, high_ref, cols, *, tile, vocab, rows):
    j = pl.program_id(0)
    half = low_ref.shape[0]

    @pl.when(j == 0)
    def _():
        cols[...] = token_columns(own_ref[...], own_ref, ax_ref, ay_ref, ad_ref)
        dn_ref[...] = jnp.zeros(dn_ref.shape, F32)
        sums = (own_ref[...] + ax_ref[...]) + (ay_ref[...] + ad_ref[...])
        row = lax.broadcasted_iota(I32, sum_ref.shape, 0)
        sum_ref[...] = jnp.where(row == 0, sums[4:5, 0:1], sums[3:4, 0:1])

    @pl.when(j == pl.num_programs(0) - 1)
    def _():
        width = vocab - (pl.cdiv(vocab, tile) - 1) * tile
        z_ref[:, width:] = jnp.zeros((z_ref.shape[0], tile - width), F32)
        w_ref[:, width:] = jnp.zeros((w_ref.shape[0], tile - width), BF16)

    g = softmax_grad(z_ref[...], cols, j * tile)
    g_ref[...] = g
    low_ref[...] = g[:half].astype(F32)
    high_ref[...] = g[half:].astype(F32)
    for c in range(0, w_ref.shape[0], rows):
        dn_ref[:, c:c + rows] += lax.dot_general(g_ref[...], w_ref[c:c + rows, :], NT, preferred_element_type=F32)


def own_grad(z, w, auxes, slots, tile=1024, rows=1024):
    t, v = z.shape
    tail = pl.BlockSpec((t // 2, tile), lambda j: (0, jnp.maximum(j - HEAD // tile, 0)))
    h = w.shape[0]
    return call(
        functools.partial(back_body, tile=tile, vocab=v, rows=rows),
        grid=(pl.cdiv(v, tile),),
        in_specs=[pl.BlockSpec((t, tile), lambda j: (0, j)), pl.BlockSpec((h, tile), lambda j: (0, j))] + [whole((ROWS, t))] * 4,
        out_specs=[pl.BlockSpec((t, tile), lambda j: (0, j)), whole((t, h)), whole((ROWS, LANES)), tail, tail],
        out_shape=[jax.ShapeDtypeStruct((slots * t, v), BF16), jax.ShapeDtypeStruct((t, h), F32), jax.ShapeDtypeStruct((ROWS, LANES), F32)] + [jax.ShapeDtypeStruct((t // 2, v - HEAD), F32)] * 2,
        scratch_shapes=[pltpu.VMEM((t, LANES), F32)],
        cost=(2 * t * h * v, 2 * h * v + 6 * t * v),
    )(z, w, *auxes)


def remote_body(slot_ref, h0_ref, h1_ref, gain_ref, w_ref, own_ref, ax_ref, ay_ref, ad_ref, _, g_ref, n_ref, cols, *, tile, chunk):
    half = h0_ref.shape[0]

    @pl.when(pl.program_id(0) == 0)
    def _():
        n_ref[:half, :] = (h0_ref[...] * gain_ref[...].astype(F32)).astype(BF16)
        n_ref[half:, :] = (h1_ref[...] * gain_ref[...].astype(F32)).astype(BF16)
        first = lax.broadcasted_iota(I32, ax_ref.shape, 1) < half
        straight = jnp.where(first, ax_ref[...], ay_ref[...])
        crossed = pltpu.roll(jnp.where(first, ay_ref[...], ax_ref[...]), half, 1)
        picked = jnp.where(slot_ref[0] == 1, straight, jnp.where(slot_ref[0] == 2, ad_ref[...], crossed))
        cols[...] = token_columns(picked, own_ref, ax_ref, ay_ref, ad_ref)

    @pl.when(pl.program_id(0) < slot_ref[1])
    def _():
        for c in range(0, tile, chunk):
            z = jnp.dot(n_ref[...], w_ref[:, c:c + chunk], preferred_element_type=F32)
            g_ref[:, c:c + chunk] = softmax_grad(z, cols, pl.program_id(0) * tile + c)


def remote_grad(slot, width, h0, h1, gain, w, auxes, g_all, tile=768, chunk=256):
    half, h = h0.shape
    t, v = 2 * half, w.shape[1]
    return call(
        functools.partial(remote_body, tile=tile, chunk=chunk),
        grid_spec=pltpu.PrefetchScalarGridSpec(
            num_scalar_prefetch=1, grid=(pl.cdiv(v, tile),),
            in_specs=[whole((half, h)), whole((half, h)), whole((1, h)), pl.BlockSpec((h, tile), lambda j, slot_ref: (0, jnp.minimum(j, slot_ref[1] - 1)))] + [whole((ROWS, t))] * 4 + [pl.BlockSpec(memory_space=pl.ANY)],
            out_specs=[pl.BlockSpec((t, tile), lambda j, slot_ref: (slot_ref[0], jnp.minimum(j, slot_ref[1] - 1))), whole((t, h))],
            scratch_shapes=[pltpu.VMEM((t, LANES), F32)],
        ),
        out_shape=[jax.ShapeDtypeStruct(g_all.shape, BF16), jax.ShapeDtypeStruct((t, h), BF16)],
        input_output_aliases={9: 0},
        cost=(2 * t * h * v, 2 * h * v + 2 * t * v),
    )(jnp.array([slot, pl.cdiv(width, tile)], I32), h0, h1, gain, w, *auxes, g_all)


def place_body(h0_ref, h1_ref, _, g_ref):
    half = h0_ref.shape[0]
    g_ref[:half, :] = h0_ref[...].astype(BF16)
    g_ref[half:, :] = h1_ref[...].astype(BF16)


def place(h0, h1, g_all, slot, tile=1024):
    half, width = h0.shape
    part = pl.BlockSpec((half, tile), lambda j: (0, j))
    return call(
        place_body,
        grid=(pl.cdiv(width, tile),),
        in_specs=[part, part, pl.BlockSpec(memory_space=pl.ANY)],
        out_specs=pl.BlockSpec((2 * half, tile), lambda j: (slot, j + HEAD // tile)),
        out_shape=jax.ShapeDtypeStruct(g_all.shape, BF16),
        input_output_aliases={2: 0},
        cost=(4 * half * width, 12 * half * width),
    )(h0, h1, g_all)


def wgrad_first_body(at_ref, *refs, tile, chunk, pieces):
    g_ref, out_ref, nts = refs[2 * pieces], refs[-3], refs[-2:]

    @pl.when(pl.program_id(0) == 0)
    def _():
        for k in range(2):
            first = 0
            for ref in refs[k * pieces:(k + 1) * pieces]:
                size = ref.shape[0]
                nts[k][:, first:first + size] = jnp.transpose(ref[...].astype(F32)).astype(BF16)
                first += size

    for c in range(0, tile, chunk):
        out_ref[:, c:c + chunk] = jnp.dot(nts[0][...], g_ref[:, c:c + chunk], preferred_element_type=F32)


def weight_grad_first(at, ns, g, tiles, tile=1792, chunk=256):
    k, _ = g.shape
    r = k // 4
    width = tiles * tile
    states = [pl.BlockSpec((n.shape[0], r), functools.partial(lambda which, j, at_ref: (0, at_ref[which]), which)) for which in range(2) for n in ns]
    return call(
        functools.partial(wgrad_first_body, tile=tile, chunk=chunk, pieces=len(ns)),
        grid_spec=pltpu.PrefetchScalarGridSpec(
            num_scalar_prefetch=1, grid=(tiles,), in_specs=states + [pl.BlockSpec((k, tile), lambda j, at_ref: (0, j))],
            out_specs=[pl.BlockSpec((r, tile), lambda j, at_ref: (0, j)), whole((r, k)), whole((r, k))],
        ),
        out_shape=[jax.ShapeDtypeStruct((r, width), F32)] + [jax.ShapeDtypeStruct((r, k), BF16)] * 2,
        cost=(2 * r * k * width, 2 * k * width + 4 * r * width),
    )(at, *ns, *ns, g)


def wgrad_body(nt_ref, g_ref, *rest, tile, chunk, with_add, with_sums):
    out_ref = rest[-3] if with_sums else rest[-1]
    if with_sums:
        gams, (sum0_ref, sum1_ref), (gam_ref, loss_ref) = rest[1:5], rest[5:7], rest[-2:]

        @pl.when(pl.program_id(0) == 0)
        def _():
            gam_ref[...] = (gams[0][...] + gams[1][...]) + (gams[2][...] + gams[3][...])
            loss_ref[...] = jnp.broadcast_to((sum0_ref[0:1, :] + sum1_ref[0:1, :]) / sum0_ref[1:2, :], loss_ref.shape)

    for c in range(0, tile, chunk):
        part = jnp.dot(nt_ref[...], g_ref[:, c:c + chunk], preferred_element_type=F32)
        out_ref[:, c:c + chunk] = part + rest[0][:, c:c + chunk] if with_add else part


def weight_grad(nt, g, first, tiles, add=None, into=None, sums=None, tile=1792, chunk=256):
    r, k = nt.shape
    v = g.shape[1]
    width = min(v - first * tile, tiles * tile)
    ins, aliases = [nt, g], {}
    specs = [whole((r, k)), pl.BlockSpec((k, tile), lambda j: (0, j + first))]
    out_specs, out_shape = pl.BlockSpec((r, tile), lambda j: (0, j)), jax.ShapeDtypeStruct((r, width), F32)
    if add is not None:
        ins.append(add)
        specs.append(pl.BlockSpec((r, tile), lambda j: (0, j)))
        out_specs, out_shape = pl.BlockSpec((r, tile), lambda j: (0, j + first)), jax.ShapeDtypeStruct((r, v), F32)
    if into is not None:
        aliases = {len(ins): 0}
        ins.append(into)
        specs.append(pl.BlockSpec(memory_space=pl.ANY))
    if sums is not None:
        ins.extend(sums)
        specs.extend(whole(a.shape) for a in sums)
        out_specs = [out_specs, whole(sums[0].shape), whole(sums[-1].shape)]
        out_shape = [out_shape, jax.ShapeDtypeStruct(sums[0].shape, F32), jax.ShapeDtypeStruct(sums[-1].shape, F32)]
    return call(
        functools.partial(wgrad_body, tile=tile, chunk=chunk, with_add=add is not None, with_sums=sums is not None),
        grid=(tiles,),
        in_specs=specs,
        out_specs=out_specs,
        out_shape=out_shape,
        input_output_aliases=aliases,
        cost=(2 * r * k * width, 2 * k * width + 4 * r * width),
    )(*ins)


def final_body(x_ref, inv_ref, gain_ref, mine_ref, other_ref, dh_ref, gam_ref):
    inv = inv_ref[...]
    hat = x_ref[...].astype(F32) * inv
    dn = mine_ref[...] + other_ref[...]
    prod = dn * hat

    @pl.when(pl.program_id(0) == 0)
    def _():
        gam_ref[...] = jnp.zeros(gam_ref.shape, F32)

    gam_ref[...] += jnp.sum(prod.reshape(-1, ROWS, prod.shape[1]), axis=0)
    d_hat = dn * gain_ref[...].astype(F32)
    dh_ref[...] = (inv * (d_hat - hat * jnp.mean(d_hat * hat, axis=-1, keepdims=True))).astype(BF16)


def final(x, inv, gain, mine, other, block=64):
    t, h = x.shape
    rows = pl.BlockSpec((block, h), lambda j: (j, 0))
    return call(
        final_body,
        grid=(t // block,),
        in_specs=[rows, pl.BlockSpec((block, 1), lambda j: (j, 0)), whole((1, h)), rows, rows],
        out_specs=[rows, whole((ROWS, h))],
        out_shape=[jax.ShapeDtypeStruct((t, h), BF16), jax.ShapeDtypeStruct((ROWS, h), F32)],
        cost=(10 * t * h, 12 * t * h),
    )(x, inv, gain, mine, other)


def solution(mesh):
    n_dp = mesh.shape["dp"]

    def swap(v, bits):
        return lax.ppermute(v, "dp", [(i, i ^ bits) for i in range(n_dp)])

    def swap_tp(v):
        return lax.ppermute(v, "tp", [(0, 1), (1, 0)])

    def step(hidden_in, labels, loss_mask, norm_gamma, w_local):
        tp, dp = lax.axis_index("tp").reshape(1), lax.axis_index("dp").reshape(1)
        gain = norm_gamma[None, :]
        low, high, n_own, inv, rows, cnt = prep(tp, hidden_in, gain, labels[None], loss_mask[None], w_local.shape[1])
        cnt_other = swap(cnt, 1)
        x_low, y_high = swap(low, 2), swap(high, 4)
        logits, stats = own_logits(n_own, w_local, rows)
        aux = combine(tp, stats, swap_tp(stats), rows, cnt, cnt_other)
        aux_x, aux_y, aux_d = swap(aux, 2), swap(aux, 4), swap(aux, 6)
        auxes = (aux, aux_x, aux_y, aux_d)
        x_low, y_high, low, high, auxes = lax.optimization_barrier((x_low, y_high, low, high, auxes))
        d_low, d_high = swap(x_low, 4), swap(y_high, 2)
        x_high, y_low = swap(high, 2), swap(low, 4)

        g_all, dn_mine, sums, tail_low, tail_high = own_grad(logits, w_local, auxes, 4)
        dn_other = swap_tp(dn_mine)
        sums_other = swap(sums, 1)
        tail_x, tail_y = swap(tail_high, 2), swap(tail_low, 4)
        ns = [n_own]
        vocab = w_local.shape[1]
        for slot, width, h0, h1 in ((1, vocab, x_low, y_high), (2, vocab, d_low, d_high), (3, HEAD, x_high, y_low)):
            g_all, n = remote_grad(slot, width, h0, h1, gain, w_local, auxes, g_all)
            ns.append(n)
        g_all = place(tail_x, tail_y, g_all, 3)

        at = jnp.concatenate([dp ^ 1, dp])
        p1, nt_other, nt_own = weight_grad_first(at, ns, g_all, 5)
        p1 = swap(p1, 1)
        p2 = swap(weight_grad(nt_other, g_all, 5, 4), 1)
        d_hidden, gam = final(hidden_in, inv, gain, dn_mine, dn_other)
        sums = (gam, swap(gam, 2), swap(gam, 4), swap(gam, 6), sums, sums_other)
        d_w_out, gam, loss = weight_grad(nt_own, g_all, 0, 5, add=p1, sums=sums)
        d_w_out = weight_grad(nt_own, g_all, 5, 4, add=p2, into=d_w_out)
        d_gamma = jnp.sum(gam + swap(gam, 1), axis=0)
        loss = loss[0, 0]
        return (loss, d_hidden, d_w_out, d_gamma)

    return jax.shard_map(step, mesh=mesh, in_specs=(P("dp", None), P("dp"), P("dp"), P(), P(None, "tp")), out_specs=(P(), P("dp", None), P("dp", "tp"), P()), check_vma=False)
```
